32 devices in a mesh: kpt: 2 (over x), row: 8 (over z, y), col: 2 (over core).
Axes of the slice: x: 2, y: 2, z: 4, core: 2. Of those that a mesh axis runs over, the one named last changes fastest.
Arguments:
- wannier: float32 [64, 32, 1024], P('kpt', ('row', 'col')), parts along dimension 0, may hold values from -6 to 6
- pairs: int32 [384, 2], replicated, may hold values from 0 to 31, as said below
- gmap: int32 [8192], replicated, may hold values from 1 to 32767, as said below
- screened: bfloat16 [4, 2, 8192, 8192], P('kpt', None, 'row', 'col'), parts along dimension 0, may hold values from -0.046875 to 0.046875
Outputs:
- coulomb: float32 [2, 2, 768, 384], P(None, None, ('kpt', 'row', 'col')), parts along dimension 2
The draws below stay inside these ranges and needn't reach their ends.
There are 2 independent parts, one for each index of `kpt`. The reference program is written for one: setup_inputs(seed, part) draws one part's arguments, and reference() takes and returns one part's arrays. A program takes and returns all parts, laid end to end along the dimension named above; an argument that names none is the same for every part. Nothing has to cross between parts.
Inputs may be any that keep to these rules, and one draw needn't show every extreme that they name: `gmap`: 8192 distinct flat cells of the grid; cell 0 is never among them. `pairs`: in each row the first Wannier function is no greater than the second; no two rows are equal.
All inputs are finite; a program needn't handle non-finite values.
Results may differ from the reference program's by a relative error of at most 0.0082.
Values may be sent and summed in bfloat16 or wider, within the bound.
No kernel may reach another device: no remote copies, remote signals or barrier semaphores. Data moves between devices by JAX's collectives and lax.ppermute only.
A program may use at most 128 MiB of HBM per device.

```python
import jax
import jax.numpy as jnp
from jax import lax

NW = 32
GX = 32
NG = 8192
NF = 2
NP = 384
GYZ = 1024


def draw_gmap(key, part):
    order = jax.random.permutation(key, GX * GX * GX - 1)
    return (order[:NG] + 1).astype(jnp.int32)


def draw_pairs(key, part):
    upper = jnp.triu_indices(NW)
    first_all = jnp.asarray(upper[0]).astype(jnp.int32)
    second_all = jnp.asarray(upper[1]).astype(jnp.int32)
    order = jax.random.permutation(jax.random.fold_in(key, 17), first_all.shape[0])
    chosen = order[:NP]
    return jnp.stack([first_all[chosen], second_all[chosen]], axis=1).astype(jnp.int32)


def block_scale(stream_key, dims, pieces, low, largest):
    level, own = 1.0, jax.random.fold_in(stream_key, 6)
    for position, blocks in pieces:
        draws = jnp.exp(jax.random.uniform(jax.random.fold_in(own, position), (blocks,), jnp.float32, low / len(pieces), largest / len(pieces)))
        level = level * jnp.repeat(draws, dims[position] // blocks).reshape([-1 if axis == position else 1 for axis in range(len(dims))])
    return level


def gaussian(own_key, shape, width, most, shards=(), dtype=jnp.bfloat16):
    values = width * jax.random.normal(own_key, shape, jnp.float32)
    if shards:
        values = values * block_scale(own_key, shape, shards, -0.22, 0.18)
    return jnp.clip(values, -most, most).astype(dtype)


def setup_inputs(seed: int = 0, part: int = 0) -> dict:
    streams_of = jax.random.split(jax.random.key(seed), 5)
    part_splits = jax.random.split(jax.random.fold_in(streams_of[4], part), 5)
    wannier = gaussian(part_splits[0], (NW, GX, GYZ), 1.0, 6.0, ((1, 16),), jnp.float32)
    pairs = draw_pairs(jax.random.fold_in(streams_of[4], 71), part)
    gmap = draw_gmap(jax.random.fold_in(streams_of[4], 71), part)
    screened = gaussian(part_splits[3], (NF, 2, NG, NG), (2 * NG) ** -0.5, 0.046875, ((2, 8), (3, 2)))
    return dict(wannier=wannier, pairs=pairs, gmap=gmap, screened=screened)


def reference(wannier, pairs, gmap, screened):
    grid = wannier.reshape(NW, GX, GX, GX)
    density = grid[pairs[:, 0]] * grid[pairs[:, 1]]
    spectrum = jnp.fft.fftn(density, axes=(1, 2, 3), norm='ortho').reshape(NP, GX * GX * GX)
    chosen = jnp.take(spectrum, gmap, axis=1)
    rho_real = jnp.real(chosen).astype(jnp.bfloat16)
    rho_imag = jnp.imag(chosen).astype(jnp.bfloat16)
    left_real = rho_real.astype(jnp.float32)
    left_imag = rho_imag.astype(jnp.float32)
    highest = lax.Precision.HIGHEST
    results = []
    for frequency in range(NF):
        w_real = screened[frequency, 0]
        w_imag = screened[frequency, 1]
        mixed_real = jnp.dot(w_real, rho_real.T, preferred_element_type=jnp.float32) - jnp.dot(w_imag, rho_imag.T, preferred_element_type=jnp.float32)
        mixed_imag = jnp.dot(w_real, rho_imag.T, preferred_element_type=jnp.float32) + jnp.dot(w_imag, rho_real.T, preferred_element_type=jnp.float32)
        u_real = jnp.dot(left_real, mixed_real, precision=highest) + jnp.dot(left_imag, mixed_imag, precision=highest)
        u_imag = jnp.dot(left_real, mixed_imag, precision=highest) - jnp.dot(left_imag, mixed_real, precision=highest)
        results.append(jnp.stack([u_real, u_imag], axis=0))
    return jnp.stack(results, axis=0) / jnp.sqrt(jnp.float32(NG))
```

```python
import functools
import math

import jax
import jax.numpy as jnp
import numpy as np
from jax import lax
from jax.experimental import pallas as pl
from jax.experimental.pallas import tpu as pltpu
from jax.sharding import PartitionSpec as P

BF = jnp.bfloat16
F32 = jnp.float32
SCALE = 1.62455
VMEM_BYTES = 67_043_328


def stage_tables(side):
    half = side // 2 + 1
    positions = np.arange(side)
    angles = 2.0 * np.pi * (np.outer(positions, positions) % side) / side
    cosine, sine = SCALE * np.cos(angles), SCALE * np.sin(angles)
    z_table = np.zeros((half, 2, 8, 8, side))
    for y in range(8):
        z_table[:, 0, y, y, :] = cosine[:half]
        z_table[:, 1, y, y, :] = -sine[:half]
    line = np.zeros((side, 2, side, 2))
    line[:, 0, :, 0] = cosine
    line[:, 0, :, 1] = sine
    line[:, 1, :, 0] = -sine
    line[:, 1, :, 1] = cosine
    y_one = line.reshape(side // 4, 4, 2, side // 8, 8, 2).transpose(0, 2, 1, 3, 5, 4)
    y_one = y_one.reshape(2 * side, 2 * side)
    x_four = np.einsum("koni,ab->okanib", line, np.eye(4)).reshape(8 * side, 8 * side)
    z_table = z_table.reshape(16 * half, 8 * side)
    tables = (z_table, np.kron(np.eye(4), y_one), y_one, x_four)
    return [jnp.asarray(table.astype(np.float32)).astype(BF) for table in tables]


def dot_nt(a, b):
    return lax.dot_general(a, b, (((1,), (1,)), ((), ())), preferred_element_type=F32)


def dot_nn(a, b):
    return lax.dot_general(a, b, (((1,), (0,)), ((), ())), preferred_element_type=F32)


def dot_tn(a, b):
    return lax.dot_general(a, b, (((0,), (0,)), ((), ())), preferred_element_type=F32)


def log2(n):
    return n.bit_length() - 1


def pair_kernel(side, planes, rows, norm, info, cells, signs, *refs):
    pieces = refs[: 2 * rows]
    picks, zt, yt, ys, xt, send, keep, wann, mid1, mid2, spec, stage, sems = refs[2 * rows :]
    half = side // 2 + 1
    me_row, me_col = info[0], info[1]
    lanes = mid2.shape[-1]
    own = lanes * 3 // 4

    copies = [
        pltpu.make_async_copy(piece, wann.at[pl.ds(index * planes, planes)], sems.at[index])
        for index, piece in enumerate(pieces)
    ]
    for copy in copies:
        copy.start()
    for copy in copies:
        copy.wait()

    def plane_pair(xp, carry):
        for h in range(2):
            x = 2 * xp + h
            from_row = lax.shift_right_logical(x, log2(2 * planes))
            from_col = lax.shift_right_logical(x, log2(planes)) & 1
            place = ((from_col ^ me_col) * rows + (from_row ^ me_row)) * planes
            plane = wann[place + (x & (planes - 1))]
            high = plane.astype(BF)
            low = (plane - high.astype(F32)).astype(BF)
            both = dot_nn(picks[...], jnp.concatenate([high, low], axis=0))
            density = (both[:own] * both[own:]).astype(BF)
            density = jnp.concatenate([density, density[lanes // 2 : own]], axis=0)
            for t in range(side // 8):
                lines = dot_nt(zt[...], density[:, t * 8 * side : (t + 1) * 8 * side])
                mid1[h, :, t] = lines.astype(BF).reshape(half, 16, lanes)
        for q in range(half // 4 + 1):
            parts = []
            for h in range(2):
                if q < half // 4:
                    lines = mid1[h, 4 * q : 4 * q + 4].reshape(8 * side, lanes)
                    parts.append(dot_nn(yt[...], lines))
                else:
                    parts.append(dot_nn(ys[...], mid1[h, half - 1].reshape(2 * side, lanes)))
            groups = parts[0].shape[0] // 8
            joined = jnp.concatenate([p.reshape(groups, 8, lanes) for p in parts], axis=1)
            mid2[pl.ds(q * side, groups), xp] = joined.astype(BF)
        return carry

    lax.fori_loop(0, side // 2, plane_pair, 0)

    left = lax.broadcasted_iota(jnp.int32, (1, 128), 1) < 64

    def column(kq, carry):
        lines = dot_nn(xt[...], mid2[kq].reshape(8 * side, lanes))
        n = 4 * side
        re, im = lines[:n], lines[n:]
        last = jnp.where(left, re[:, 128:], im[:, 128:])
        spec[pl.ds(kq * n, n), 0, :] = jnp.concatenate([re[:, :128], im[:, :128], last], axis=1)
        return carry

    lax.fori_loop(0, mid2.shape[0], column, 0, unroll=2)

    block = stage.shape[0]
    lane = lax.broadcasted_iota(jnp.int32, (1, 384), 1)
    imag = ((lane >= 128) & (lane < 256)) | (lane >= 320)

    def gather_into(out, first):
        def step(b, carry):
            base = first + b * block
            for j in range(block):
                row = spec[cells[base + j]]
                stage[j] = row * jnp.where(imag, signs[base + j], norm)
            out[pl.ds(pl.multiple_of(b * block, block), block), :] = stage[:, 0, :].astype(BF)
            return carry

        lax.fori_loop(0, out.shape[0] // block, step, 0)

    gather_into(send, 0)
    gather_into(keep, send.shape[0])


def pair_coefficients(info, cells, signs, pieces, picks, side, norm, send_rows):
    keep_rows = cells.shape[0] - send_rows
    planes, members = pieces[0].shape[:2]
    half = side // 2 + 1
    lanes = 256
    smem = pl.BlockSpec(memory_space=pltpu.SMEM)
    vmem = pl.BlockSpec(memory_space=pltpu.VMEM)
    return pl.pallas_call(
        functools.partial(pair_kernel, side, planes, len(pieces) // 2, norm),
        out_shape=(
            jax.ShapeDtypeStruct((send_rows, 384), BF),
            jax.ShapeDtypeStruct((keep_rows, 384), BF),
        ),
        in_specs=[smem] * 3 + [pl.BlockSpec(memory_space=pl.ANY)] * len(pieces) + [vmem] * 5,
        out_specs=(vmem, vmem),
        scratch_shapes=[
            pltpu.VMEM((side, members, side * side), F32),
            pltpu.VMEM((2, half, side // 8, 16, lanes), BF),
            pltpu.VMEM((half * side // 4, side // 2, 16, lanes), BF),
            pltpu.VMEM((half * side * side, 1, 384), F32),
            pltpu.VMEM((32, 1, 384), F32),
            pltpu.SemaphoreType.DMA((len(pieces),)),
        ],
        compiler_params=pltpu.CompilerParams(vmem_limit_bytes=VMEM_BYTES),
        cost_estimate=pl.CostEstimate(
            flops=30_000_000_000, bytes_accessed=12_000_000, transcendentals=0
        ),
        name="pair_coefficients",
    )(info, cells, signs, *pieces, picks, *stage_tables(side))


def ordered(mine, theirs, is_first):
    first = jnp.where(is_first, mine, theirs)
    second = jnp.where(is_first, theirs, mine)
    left = lax.broadcasted_iota(jnp.int32, (1, 128), 1) < 64
    a, b = first[:, 256:], second[:, 256:]
    re = jnp.concatenate(
        [first[:, :128], second[:, :128], jnp.where(left, a, pltpu.roll(b, 64, 1))], axis=1
    )
    im = jnp.concatenate(
        [first[:, 128:256], second[:, 128:256], jnp.where(left, pltpu.roll(a, 64, 1), b)], axis=1
    )
    return re, im


def coulomb_kernel(
    steps, shares, scale, info, keep, send_g, recv, recv_g, w, mine, other, r0, r1, lhs, mixed
):
    step = pl.program_id(1)
    is_first = info[1] == 0
    pairs = r0.shape[1] // 2

    @pl.when((pl.program_id(0) == 0) & (step == 0))
    def _():
        chunk = 256

        def build(i, carry):
            at = pl.ds(pl.multiple_of(i * chunk, chunk), chunk)
            re, im = ordered(keep[at, :].astype(F32), recv[at, :].astype(F32), is_first)
            r0[at, :] = jnp.concatenate([re, im], axis=1).astype(BF)
            r1[at, :] = jnp.concatenate([-im, re], axis=1).astype(BF)
            return carry

        lax.fori_loop(0, keep.shape[0] // chunk, build, 0)

        def build_left(i, carry):
            at = pl.ds(pl.multiple_of(i * chunk, chunk), chunk)
            re, im = ordered(send_g[at, :].astype(F32), recv_g[at, :].astype(F32), is_first)
            lhs[at, :] = jnp.concatenate([re, im], axis=1).astype(BF)
            return carry

        lax.fori_loop(0, lhs.shape[0] // chunk, build_left, 0)

    tile = w.shape[2]
    product = dot_nn(w[0, 0], r0[...]) + dot_nn(w[0, 1], r1[...])
    mixed[pl.ds(pl.multiple_of(step * tile, tile), tile), :] = product.astype(BF)

    @pl.when(step == steps - 1)
    def _():
        re_rows = dot_tn(lhs[:, :pairs], mixed[...])
        im_rows = dot_tn(lhs[:, pairs:], mixed[...])
        u = (
            (re_rows[:, :pairs] + im_rows[:, pairs:]) * scale,
            (re_rows[:, pairs:] - im_rows[:, :pairs]) * scale,
        )
        n = pairs // shares

        def put(even, odd):
            for part in range(2):
                for s in range(shares):
                    target = odd if s % 2 else even
                    target[s // 2, 0, part] = u[part][s * n : (s + 1) * n]

        @pl.when(is_first)
        def _():
            put(mine, other)

        @pl.when(jnp.logical_not(is_first))
        def _():
            put(other, mine)


def coulomb_partial(info, keep, send, recv, screened, rows, scale):
    freqs, _, g_rows, h_rows = screened.shape
    pairs = keep.shape[1]
    tile = min(256, g_rows)
    steps = g_rows // tile
    shares = 2 * rows
    shape = (rows, freqs, 2, pairs // shares, pairs)
    once = pl.Buffered(1)

    def fixed(n, index):
        return pl.BlockSpec((n, pairs), lambda f, i: (index, 0), pipeline_mode=once)

    out_spec = pl.BlockSpec((rows, 1) + shape[2:], lambda f, i: (0, f, 0, 0, 0))
    return pl.pallas_call(
        functools.partial(coulomb_kernel, steps, shares, scale),
        grid=(freqs, steps),
        out_shape=(jax.ShapeDtypeStruct(shape, F32),) * 2,
        in_specs=[
            pl.BlockSpec(memory_space=pltpu.SMEM),
            fixed(h_rows, 0),
            fixed(g_rows, h_rows // g_rows),
            fixed(h_rows, 0),
            fixed(g_rows, h_rows // g_rows),
            pl.BlockSpec((1, 2, tile, h_rows), lambda f, i: (f, 0, i, 0)),
        ],
        out_specs=(out_spec, out_spec),
        scratch_shapes=[
            pltpu.VMEM((h_rows, 2 * pairs), BF),
            pltpu.VMEM((h_rows, 2 * pairs), BF),
            pltpu.VMEM((g_rows, 2 * pairs), BF),
            pltpu.VMEM((g_rows, 2 * pairs), BF),
        ],
        compiler_params=pltpu.CompilerParams(vmem_limit_bytes=VMEM_BYTES),
        cost_estimate=pl.CostEstimate(
            flops=28_000_000_000, bytes_accessed=45_000_000, transcendentals=0
        ),
        name="coulomb_partial",
    )(info, keep, send, recv, recv, screened)


def cell_table(gmap, side, norm):
    kx, ky, kz = gmap // (side * side), gmap // side % side, gmap % side
    mirrored = kz > side // 2
    kx, ky, kz = (jnp.where(mirrored, -k % side, k) for k in (kx, ky, kz))
    cells = ((kz * (side // 4) + ky // 4) * side + kx) * 4 + ky % 4
    return cells, jnp.where(mirrored, -norm, norm).astype(F32)


def shards(rows, cols, wannier, pairs, gmap, screened):
    members, planes, grid_cells = wannier.shape
    side = math.isqrt(grid_cells)
    count = pairs.shape[0]
    waves = gmap.shape[0]
    g_rows, h_rows = screened.shape[2:]
    row, col = lax.axis_index("row"), lax.axis_index("col")
    info = jnp.stack([row, col]).astype(jnp.int32)
    swap = [(0, 1), (1, 0)]

    local = wannier.transpose(1, 0, 2)
    same = [local]
    for shift in range(1, rows):
        same.append(lax.ppermute(local, "row", [(i, i ^ shift) for i in range(rows)]))
    cross = [lax.ppermute(piece, "col", swap) for piece in same]

    wide = count // 3
    first = lax.dynamic_slice_in_dim(pairs, col * wide, wide, 0)
    last = lax.dynamic_slice_in_dim(pairs, 2 * wide + col * (wide // 2), wide // 2, 0)
    owned = jnp.concatenate([first, last], axis=0).T.reshape(-1, 1)
    picks = (owned == jnp.arange(2 * members, dtype=jnp.int32)[None, :] % members).astype(BF)

    norm = 1.0 / (math.sqrt(side**3) * SCALE**3)
    cells, signs = cell_table(gmap, side, norm)

    def arranged(table):
        theirs = lax.dynamic_slice_in_dim(table, (1 - col) * h_rows, h_rows)
        block = lax.dynamic_slice_in_dim(table, row * g_rows, g_rows)
        ours = lax.dynamic_slice_in_dim(table, col * h_rows, h_rows)
        return jnp.concatenate([theirs, block, ours])

    send, keep = pair_coefficients(
        info, arranged(cells), arranged(signs), same + cross, picks, side, norm, h_rows + g_rows
    )
    recv = lax.ppermute(send, "col", swap)
    mine, other = coulomb_partial(
        info, keep, send, recv, screened, rows, 1.0 / math.sqrt(waves)
    )
    chip = mine + lax.ppermute(other, "col", swap)
    spread = lax.all_to_all(chip.astype(BF), "row", split_axis=0, concat_axis=0, tiled=True)
    return jnp.sum(spread.astype(F32), axis=0)


def solution(mesh):
    rows, cols = mesh.shape["row"], mesh.shape["col"]
    return jax.shard_map(
        functools.partial(shards, rows, cols),
        mesh=mesh,
        in_specs=(P("kpt", ("row", "col"), None), P(), P(), P("kpt", None, "row", "col")),
        out_specs=P(None, None, ("kpt", "row", "col"), None),
        check_vma=False,
    )
```

```python
import functools
import math

import jax
import jax.numpy as jnp
import numpy as np
from jax import lax
from jax.experimental import pallas as pl
from jax.experimental.pallas import tpu as pltpu
from jax.sharding import PartitionSpec as P

BF = jnp.bfloat16
F32 = jnp.float32
SCALE = 1.62455
VMEM_BYTES = 67_043_328


def stage_tables(side):
    half = side // 2 + 1
    positions = np.arange(side)
    angles = 2.0 * np.pi * (np.outer(positions, positions) % side) / side
    cosine, sine = SCALE * np.cos(angles), SCALE * np.sin(angles)
    z_table = np.zeros((half, 2, 8, 8, side))
    for y in range(8):
        z_table[:, 0, y, y, :] = cosine[:half]
        z_table[:, 1, y, y, :] = -sine[:half]
    line = np.zeros((side, 2, side, 2))
    line[:, 0, :, 0] = cosine
    line[:, 0, :, 1] = sine
    line[:, 1, :, 0] = -sine
    line[:, 1, :, 1] = cosine
    y_one = line.reshape(side // 4, 4, 2, side // 8, 8, 2).transpose(0, 2, 1, 3, 5, 4)
    y_one = y_one.reshape(2 * side, 2 * side)
    x_four = np.einsum("koni,ab->okanib", line, np.eye(4)).reshape(8 * side, 8 * side)
    z_table = z_table.reshape(16 * half, 8 * side)
    tables = (z_table, np.kron(np.eye(4), y_one), y_one, x_four)
    return [jnp.asarray(table.astype(np.float32)).astype(BF) for table in tables]


def dot_nt(a, b):
    return lax.dot_general(a, b, (((1,), (1,)), ((), ())), preferred_element_type=F32)


def dot_nn(a, b):
    return lax.dot_general(a, b, (((1,), (0,)), ((), ())), preferred_element_type=F32)


def dot_tn(a, b):
    return lax.dot_general(a, b, (((0,), (0,)), ((), ())), preferred_element_type=F32)


def log2(n):
    return n.bit_length() - 1


def pair_kernel(side, planes, rows, norm, info, cells, signs, *refs):
    pieces = refs[: 2 * rows]
    picks, zt, yt, ys, xt, send, keep, wann, mid1, mid2, spec, stage, sems = refs[2 * rows :]
    half = side // 2 + 1
    me_row, me_col = info[0], info[1]
    lanes = mid2.shape[-1]
    own = lanes * 3 // 4

    copies = [
        pltpu.make_async_copy(piece, wann.at[pl.ds(index * planes, planes)], sems.at[index])
        for index, piece in enumerate(pieces)
    ]
    for copy in copies:
        copy.start()
    for copy in copies:
        copy.wait()

    def plane_pair(xp, carry):
        for h in range(2):
            x = 2 * xp + h
            from_row = lax.shift_right_logical(x, log2(2 * planes))
            from_col = lax.shift_right_logical(x, log2(planes)) & 1
            place = ((from_col ^ me_col) * rows + (from_row ^ me_row)) * planes
            plane = wann[place + (x & (planes - 1))]
            high = plane.astype(BF)
            low = (plane - high.astype(F32)).astype(BF)
            both = dot_nn(picks[...], jnp.concatenate([high, low], axis=0))
            density = (both[:own] * both[own:]).astype(BF)
            density = jnp.concatenate([density, density[lanes // 2 : own]], axis=0)
            for t in range(side // 8):
                lines = dot_nt(zt[...], density[:, t * 8 * side : (t + 1) * 8 * side])
                mid1[h, :, t] = lines.astype(BF).reshape(half, 16, lanes)
        for q in range(half // 4 + 1):
            parts = []
            for h in range(2):
                if q < half // 4:
                    lines = mid1[h, 4 * q : 4 * q + 4].reshape(8 * side, lanes)
                    parts.append(dot_nn(yt[...], lines))
                else:
                    parts.append(dot_nn(ys[...], mid1[h, half - 1].reshape(2 * side, lanes)))
            groups = parts[0].shape[0] // 8
            joined = jnp.concatenate([p.reshape(groups, 8, lanes) for p in parts], axis=1)
            mid2[pl.ds(q * side, groups), xp] = joined.astype(BF)
        return carry

    lax.fori_loop(0, side // 2, plane_pair, 0)

    left = lax.broadcasted_iota(jnp.int32, (1, 128), 1) < 64

    def column(kq, carry):
        lines = dot_nn(xt[...], mid2[kq].reshape(8 * side, lanes))
        n = 4 * side
        re, im = lines[:n], lines[n:]
        thirds = (re[:, :128], im[:, :128], jnp.where(left, re[:, 128:], im[:, 128:]))
        for third in range(3):
            for odd in range(2):
                at = pl.ds(kq * 3 * n + 2 * third + odd, n // 2, stride=6)
                spec[at, :] = thirds[third][odd * n // 2 : (odd + 1) * n // 2]
        return carry

    lax.fori_loop(0, mid2.shape[0], column, 0, unroll=4)

    block = 128

    def gather_into(out, first):
        def step(b, carry):
            base = first + b * block
            for j in range(block):
                odd, even = divmod(j, block // 2)
                stage[pl.ds(6 * even + odd, 3, stride=2), :] = spec[pl.ds(cells[base + j], 3, stride=2), :]
            sign = jnp.transpose(jnp.broadcast_to(signs[pl.ds(first // block + b, 1), :], (block, block)))
            plain = jnp.full_like(sign, norm)
            scales = (plain, sign, jnp.where(left, plain, sign))
            at = pl.ds(pl.multiple_of(b * block, block), block)
            for third in range(3):
                halves = [stage[pl.ds(2 * third + odd, block // 2, stride=6), :] for odd in range(2)]
                whole = jnp.concatenate(halves, axis=0) * scales[third]
                out[at, third * 128 : (third + 1) * 128] = whole.astype(BF)
            return carry

        lax.fori_loop(0, out.shape[0] // block, step, 0)

    gather_into(send, 0)
    gather_into(keep, send.shape[0])


def pair_coefficients(info, cells, signs, pieces, picks, side, norm, send_rows):
    keep_rows = cells.shape[0] - send_rows
    planes, members = pieces[0].shape[:2]
    half = side // 2 + 1
    lanes = 256
    smem = pl.BlockSpec(memory_space=pltpu.SMEM)
    vmem = pl.BlockSpec(memory_space=pltpu.VMEM)
    return pl.pallas_call(
        functools.partial(pair_kernel, side, planes, len(pieces) // 2, norm),
        out_shape=(
            jax.ShapeDtypeStruct((send_rows, 384), BF),
            jax.ShapeDtypeStruct((keep_rows, 384), BF),
        ),
        in_specs=[smem, smem, vmem] + [pl.BlockSpec(memory_space=pl.ANY)] * len(pieces) + [vmem] * 5,
        out_specs=(vmem, vmem),
        scratch_shapes=[
            pltpu.VMEM((side, members, side * side), F32),
            pltpu.VMEM((2, half, side // 8, 16, lanes), BF),
            pltpu.VMEM((half * side // 4, side // 2, 16, lanes), BF),
            pltpu.VMEM((half * side * side * 3, 128), F32),
            pltpu.VMEM((3 * 128, 128), F32),
            pltpu.SemaphoreType.DMA((len(pieces),)),
        ],
        compiler_params=pltpu.CompilerParams(vmem_limit_bytes=VMEM_BYTES),
        cost_estimate=pl.CostEstimate(
            flops=30_000_000_000, bytes_accessed=12_000_000, transcendentals=0
        ),
        name="pair_coefficients",
    )(info, cells, signs.reshape(-1, 128), *pieces, picks, *stage_tables(side))


def ordered(mine, theirs, is_first):
    first = jnp.where(is_first, mine, theirs)
    second = jnp.where(is_first, theirs, mine)
    left = lax.broadcasted_iota(jnp.int32, (1, 128), 1) < 64
    a, b = first[:, 256:], second[:, 256:]
    re = jnp.concatenate(
        [first[:, :128], second[:, :128], jnp.where(left, a, pltpu.roll(b, 64, 1))], axis=1
    )
    im = jnp.concatenate(
        [first[:, 128:256], second[:, 128:256], jnp.where(left, pltpu.roll(a, 64, 1), b)], axis=1
    )
    return re, im


def coulomb_kernel(
    steps, shares, scale, info, keep, send_g, recv, recv_g, w, mine, other, r0, r1, lhs, mixed
):
    step = pl.program_id(1)
    is_first = info[1] == 0
    pairs = r0.shape[1] // 2

    @pl.when((pl.program_id(0) == 0) & (step == 0))
    def _():
        chunk = 256

        def build(i, carry):
            at = pl.ds(pl.multiple_of(i * chunk, chunk), chunk)
            re, im = ordered(keep[at, :].astype(F32), recv[at, :].astype(F32), is_first)
            r0[at, :] = jnp.concatenate([re, im], axis=1).astype(BF)
            r1[at, :] = jnp.concatenate([-im, re], axis=1).astype(BF)
            return carry

        lax.fori_loop(0, keep.shape[0] // chunk, build, 0)

        def build_left(i, carry):
            at = pl.ds(pl.multiple_of(i * chunk, chunk), chunk)
            re, im = ordered(send_g[at, :].astype(F32), recv_g[at, :].astype(F32), is_first)
            lhs[at, :] = jnp.concatenate([re, im], axis=1).astype(BF)
            return carry

        lax.fori_loop(0, lhs.shape[0] // chunk, build_left, 0)

    tile = w.shape[2]
    product = dot_nn(w[0, 0], r0[...]) + dot_nn(w[0, 1], r1[...])
    mixed[pl.ds(pl.multiple_of(step * tile, tile), tile), :] = product.astype(BF)

    @pl.when(step == steps - 1)
    def _():
        re_rows = dot_tn(lhs[:, :pairs], mixed[...])
        im_rows = dot_tn(lhs[:, pairs:], mixed[...])
        u = (
            (re_rows[:, :pairs] + im_rows[:, pairs:]) * scale,
            (re_rows[:, pairs:] - im_rows[:, :pairs]) * scale,
        )
        n = pairs // shares

        def put(even, odd):
            for part in range(2):
                for s in range(shares):
                    target = odd if s % 2 else even
                    target[s // 2, 0, part] = u[part][s * n : (s + 1) * n]

        @pl.when(is_first)
        def _():
            put(mine, other)

        @pl.when(jnp.logical_not(is_first))
        def _():
            put(other, mine)


def coulomb_partial(info, keep, send, recv, screened, rows, scale):
    freqs, _, g_rows, h_rows = screened.shape
    pairs = keep.shape[1]
    tile = min(256, g_rows)
    steps = g_rows // tile
    shares = 2 * rows
    shape = (rows, freqs, 2, pairs // shares, pairs)
    once = pl.Buffered(1)

    def fixed(n, index):
        return pl.BlockSpec((n, pairs), lambda f, i: (index, 0), pipeline_mode=once)

    out_spec = pl.BlockSpec((rows, 1) + shape[2:], lambda f, i: (0, f, 0, 0, 0))
    return pl.pallas_call(
        functools.partial(coulomb_kernel, steps, shares, scale),
        grid=(freqs, steps),
        out_shape=(jax.ShapeDtypeStruct(shape, F32),) * 2,
        in_specs=[
            pl.BlockSpec(memory_space=pltpu.SMEM),
            fixed(h_rows, 0),
            fixed(g_rows, h_rows // g_rows),
            fixed(h_rows, 0),
            fixed(g_rows, h_rows // g_rows),
            pl.BlockSpec((1, 2, tile, h_rows), lambda f, i: (f, 0, i, 0)),
        ],
        out_specs=(out_spec, out_spec),
        scratch_shapes=[
            pltpu.VMEM((h_rows, 2 * pairs), BF),
            pltpu.VMEM((h_rows, 2 * pairs), BF),
            pltpu.VMEM((g_rows, 2 * pairs), BF),
            pltpu.VMEM((g_rows, 2 * pairs), BF),
        ],
        compiler_params=pltpu.CompilerParams(vmem_limit_bytes=VMEM_BYTES),
        cost_estimate=pl.CostEstimate(
            flops=28_000_000_000, bytes_accessed=45_000_000, transcendentals=0
        ),
        name="coulomb_partial",
    )(info, keep, send, recv, recv, screened)


def cell_table(gmap, side, norm):
    kx, ky, kz = gmap // (side * side), gmap // side % side, gmap % side
    mirrored = kz > side // 2
    kx, ky, kz = (jnp.where(mirrored, -k % side, k) for k in (kx, ky, kz))
    place = kx * 4 + ky % 4
    cells = (kz * (side // 4) + ky // 4) * 12 * side + place % (2 * side) * 6 + place // (2 * side)
    return cells, jnp.where(mirrored, -norm, norm).astype(F32)


def shards(rows, cols, wannier, pairs, gmap, screened):
    members, planes, grid_cells = wannier.shape
    side = math.isqrt(grid_cells)
    count = pairs.shape[0]
    waves = gmap.shape[0]
    g_rows, h_rows = screened.shape[2:]
    row, col = lax.axis_index("row"), lax.axis_index("col")
    info = jnp.stack([row, col]).astype(jnp.int32)
    swap = [(0, 1), (1, 0)]

    local = wannier.transpose(1, 0, 2)
    same = [local]
    for bit in reversed(range(log2(rows))):
        hop = [(i, i ^ (1 << bit)) for i in range(rows)]
        same += [lax.ppermute(piece, "row", hop) for piece in same]
    order = [0]
    for bit in reversed(range(log2(rows))):
        order += [index ^ (1 << bit) for index in order]
    same = [same[order.index(shift)] for shift in range(rows)]
    cross = [lax.ppermute(piece, "col", swap) for piece in same]

    wide = count // 3
    first = lax.dynamic_slice_in_dim(pairs, col * wide, wide, 0)
    last = lax.dynamic_slice_in_dim(pairs, 2 * wide + col * (wide // 2), wide // 2, 0)
    owned = jnp.concatenate([first, last], axis=0).T.reshape(-1, 1)
    picks = (owned == jnp.arange(2 * members, dtype=jnp.int32)[None, :] % members).astype(BF)

    norm = 1.0 / (math.sqrt(side**3) * SCALE**3)
    cells, signs = cell_table(gmap, side, norm)

    def arranged(table):
        theirs = lax.dynamic_slice_in_dim(table, (1 - col) * h_rows, h_rows)
        block = lax.dynamic_slice_in_dim(table, row * g_rows, g_rows)
        ours = lax.dynamic_slice_in_dim(table, col * h_rows, h_rows)
        return jnp.concatenate([theirs, block, ours])

    send, keep = pair_coefficients(
        info, arranged(cells), arranged(signs), same + cross, picks, side, norm, h_rows + g_rows
    )
    recv = lax.ppermute(send, "col", swap)
    mine, other = coulomb_partial(
        info, keep, send, recv, screened, rows, 1.0 / math.sqrt(waves)
    )
    chip = mine + lax.ppermute(other, "col", swap)
    spread = lax.all_to_all(chip.astype(BF), "row", split_axis=0, concat_axis=0, tiled=True)
    return jnp.sum(spread.astype(F32), axis=0)


def solution(mesh):
    rows, cols = mesh.shape["row"], mesh.shape["col"]
    return jax.shard_map(
        functools.partial(shards, rows, cols),
        mesh=mesh,
        in_specs=(P("kpt", ("row", "col"), None), P(), P(), P("kpt", None, "row", "col")),
        out_specs=P(None, None, ("kpt", "row", "col"), None),
        check_vma=False,
    )
```

```python
import functools
import math

import jax
import jax.numpy as jnp
import numpy as np
from jax import lax
from jax.experimental import pallas as pl
from jax.experimental.pallas import tpu as pltpu
from jax.sharding import PartitionSpec as P

BF = jnp.bfloat16
F32 = jnp.float32
SCALE = 1.62455
VMEM_BYTES = 67_043_328
CHUNKS = 4


def stage_tables(side):
    half = side // 2 + 1
    positions = np.arange(side)
    angles = 2.0 * np.pi * (np.outer(positions, positions) % side) / side
    cosine, sine = SCALE * np.cos(angles), SCALE * np.sin(angles)
    z_table = np.zeros((half, 2, 8, 8, side))
    for y in range(8):
        z_table[:, 0, y, y, :] = cosine[:half]
        z_table[:, 1, y, y, :] = -sine[:half]
    line = np.zeros((side, 2, side, 2))
    line[:, 0, :, 0] = cosine
    line[:, 0, :, 1] = sine
    line[:, 1, :, 0] = -sine
    line[:, 1, :, 1] = cosine
    y_one = line.reshape(side // 4, 4, 2, side // 8, 8, 2).transpose(0, 2, 1, 3, 5, 4)
    y_one = y_one.reshape(2 * side, 2 * side)
    x_four = np.einsum("koni,ab->okanib", line, np.eye(4)).reshape(8 * side, 8 * side)
    z_table = z_table.reshape(16 * half, 8 * side)
    tables = (z_table, np.kron(np.eye(4), y_one), y_one, x_four)
    return [jnp.asarray(table.astype(np.float32)).astype(BF) for table in tables]


def dot_nt(a, b):
    return lax.dot_general(a, b, (((1,), (1,)), ((), ())), preferred_element_type=F32)


def dot_nn(a, b):
    return lax.dot_general(a, b, (((1,), (0,)), ((), ())), preferred_element_type=F32)


def log2(n):
    return n.bit_length() - 1


def transform_planes(side, planes, my_col, pieces, tables, wann, mid1, sems, sink):
    picks, zt, yt, ys = [held for _, held in tables]
    half = side // 2 + 1
    lanes = mid1.shape[-1]
    own = lanes * 3 // 4
    shifts = len(pieces) // 2

    for index, piece in enumerate(pieces):
        at = pl.ds(index * planes, planes)
        pltpu.make_async_copy(piece, wann.at[at], sems.at[index]).start()
    loads = [
        pltpu.make_async_copy(table, held, sems.at[len(pieces) + index])
        for index, (table, held) in enumerate(tables)
    ]
    for load in loads:
        load.start()

    def arrived(index):
        at = pl.ds(index * planes, planes)
        pltpu.make_async_copy(pieces[0], wann.at[at], sems.at[index]).wait()

    def plane_pair(pair, carry):
        for h in range(2):
            x = 2 * pair + h
            shift = lax.shift_right_logical(x, log2(2 * planes))
            from_col = lax.shift_right_logical(x, log2(planes)) & 1
            index = (from_col ^ my_col) * shifts + shift
            if planes <= 2:
                if h % planes == 0:
                    arrived(index)
            else:
                pl.when(x & (planes - 1) == 0)(functools.partial(arrived, index))
            plane = wann[index * planes + (x & (planes - 1))]
            high = plane.astype(BF)
            low = (plane - high.astype(F32)).astype(BF)
            both = dot_nn(picks[...], jnp.concatenate([high, low], axis=0))
            density = (both[:own] * both[own:]).astype(BF)
            density = jnp.concatenate([density, density[lanes // 2 : own]], axis=0)
            for t in range(side // 8):
                lines = dot_nt(zt[...], density[:, t * 8 * side : (t + 1) * 8 * side])
                mid1[h, :, t] = lines.astype(BF).reshape(half, 16, lanes)
        target = sink(pair)
        for q in range(half // 4 + 1):
            parts = []
            for h in range(2):
                if q < half // 4:
                    lines = mid1[h, 4 * q : 4 * q + 4].reshape(8 * side, lanes)
                    parts.append(dot_nn(yt[...], lines))
                else:
                    parts.append(dot_nn(ys[...], mid1[h, half - 1].reshape(2 * side, lanes)))
            groups = parts[0].shape[0] // 8
            joined = jnp.concatenate([p.reshape(groups, 8, lanes) for p in parts], axis=1)
            target[pl.ds(q * side, groups)] = joined.astype(BF)
        return carry

    return plane_pair, loads


def plane_kernel(side, planes, info, *refs):
    pieces = refs[:-14]
    out, *held, wann, mid1, ready, sems, out_sems = refs[-10:]
    tables = list(zip(refs[-14:-10], held))
    pairs = len(pieces) // 2 * planes

    def put(pair):
        slot = pair & 1
        return pltpu.make_async_copy(ready.at[slot], out.at[pair], out_sems.at[slot])

    plane_pair, loads = transform_planes(
        side, planes, info[1], pieces, tables, wann, mid1, sems, lambda p: ready.at[p & 1]
    )
    for load in loads:
        load.wait()

    def step(pair, carry):
        pl.when(pair >= 2)(lambda: put(pair - 2).wait())
        plane_pair(pair, carry)
        put(pair).start()
        return carry

    lax.fori_loop(0, pairs, step, 0)
    for pair in range(max(pairs - 2, 0), pairs):
        put(pair).wait()


def plane_lines(info, pieces, picks, tables, side):
    planes, members = pieces[0].shape[:2]
    half = side // 2 + 1
    lanes = 256
    pairs = len(pieces) // 2 * planes
    return pl.pallas_call(
        functools.partial(plane_kernel, side, planes),
        out_shape=jax.ShapeDtypeStruct((pairs, half * side // 4, 16, lanes), BF),
        in_specs=[pl.BlockSpec(memory_space=pltpu.SMEM)]
        + [pl.BlockSpec(memory_space=pl.ANY)] * (len(pieces) + 4),
        out_specs=pl.BlockSpec(memory_space=pl.ANY),
        scratch_shapes=[pltpu.VMEM(table.shape, BF) for table in (picks, *tables)]
        + [
            pltpu.VMEM((2 * pairs, members, side * side), F32),
            pltpu.VMEM((2, half, side // 8, 16, lanes), BF),
            pltpu.VMEM((2, half * side // 4, 16, lanes), BF),
            pltpu.SemaphoreType.DMA((len(pieces) + 4,)),
            pltpu.SemaphoreType.DMA((2,)),
        ],
        compiler_params=pltpu.CompilerParams(vmem_limit_bytes=VMEM_BYTES),
        cost_estimate=pl.CostEstimate(
            flops=600_000_000 * pairs, bytes_accessed=6_000_000, transcendentals=0
        ),
        name="plane_lines",
    )(info, *pieces, picks, *tables)


def pair_kernel(side, planes, norm, early, late, info, cells, signs, *refs):
    early_lines, pieces = refs[0], refs[1:-18]
    send, keep, *held, xt, wann, mid1, mid2, spec, stages, sems = refs[-13:]
    tables = list(zip(refs[-18:-13], held + [xt]))
    lanes = mid2.shape[-1]
    own = lanes * 3 // 4

    def place(shift, rest):
        return (info[0] ^ shift) * planes + rest

    copies = []
    for pair in range(len(early) * planes):
        to = place(early[pair // planes], pair % planes)
        copies.append(
            pltpu.make_async_copy(
                early_lines.at[pair], mid2.at[:, to], sems.at[len(pieces) + 5 + pair]
            )
        )
    plane_pair, loads = transform_planes(
        side, planes, info[1], pieces, tables[:4], wann, mid1, sems,
        lambda pair: mid2.at[:, place(late[0] + lax.div(pair, planes), pair & (planes - 1))],
    )
    copies.append(pltpu.make_async_copy(*tables[4], sems.at[len(pieces) + 4]))
    for copy in copies:
        copy.start()
    for load in loads:
        load.wait()
    lax.fori_loop(0, len(late) * planes, plane_pair, 0)
    for copy in copies:
        copy.wait()

    left = lax.broadcasted_iota(jnp.int32, (1, 128), 1) < 64

    def column(kq, carry):
        lines = dot_nn(xt[...], mid2[kq].reshape(8 * side, lanes))
        n = 4 * side
        re, im = lines[:n], lines[n:]
        thirds = (re[:, :128], im[:, :128], jnp.where(left, re[:, 128:], im[:, 128:]))
        for third in range(3):
            for odd in range(2):
                at = pl.ds(kq * 3 * n + 2 * third + odd, n // 2, stride=6)
                spec[at, :] = thirds[third][odd * n // 2 : (odd + 1) * n // 2]
        return carry

    lax.fori_loop(0, mid2.shape[0], column, 0, unroll=8)

    block = 128
    deep = stages.shape[0]

    def fill(slot, base):
        for j in range(block):
            odd, even = divmod(j, block // 2)
            row = spec[pl.ds(cells[base + j], 3, stride=2), :]
            stages[slot, pl.ds(6 * even + odd, 3, stride=2), :] = row

    def drain(slot, out, b, sign):
        at = pl.ds(pl.multiple_of(b * block, block), block)
        columns = []
        for third in range(3):
            halves = [
                stages[slot, pl.ds(2 * third + odd, block // 2, stride=6), :] for odd in range(2)
            ]
            whole = jnp.concatenate(halves, axis=0) * norm
            columns.append(jnp.transpose(whole.astype(BF)))
        half_rows = block // 2
        sign = sign.astype(BF)
        out[:block, at] = columns[0]
        out[block : block + half_rows, at] = columns[2][:half_rows]
        out[own : own + block, at] = columns[1] * sign
        out[own + block :, at] = columns[2][half_rows:] * sign

    def gather_into(out, first):
        def step(i, carry):
            for slot in range(deep):
                fill(slot, first + (i * deep + slot) * block)
            for slot in range(deep):
                b = i * deep + slot
                drain(slot, out, b, signs[pl.ds(first // block + b, 1), :])
            return carry

        lax.fori_loop(0, out.shape[1] // block // deep, step, 0)

    gather_into(send, 0)
    gather_into(keep, send.shape[1])


def pair_coefficients(
    info, cells, signs, lines, pieces, picks, tables, early, late, side, norm, send_rows
):
    keep_rows = cells.shape[0] - send_rows
    planes, members = pieces[0].shape[:2]
    half = side // 2 + 1
    lanes = 256
    pairs = side // 2
    smem = pl.BlockSpec(memory_space=pltpu.SMEM)
    vmem = pl.BlockSpec(memory_space=pltpu.VMEM)
    anywhere = pl.BlockSpec(memory_space=pl.ANY)
    return pl.pallas_call(
        functools.partial(pair_kernel, side, planes, norm, early, late),
        out_shape=(
            jax.ShapeDtypeStruct((384, send_rows), BF),
            jax.ShapeDtypeStruct((384, keep_rows), BF),
        ),
        in_specs=[smem, smem, vmem] + [anywhere] * (6 + len(pieces)),
        out_specs=(vmem, vmem),
        scratch_shapes=[pltpu.VMEM(table.shape, BF) for table in (picks, *tables)]
        + [
            pltpu.VMEM((len(pieces) * planes, members, side * side), F32),
            pltpu.VMEM((2, half, side // 8, 16, lanes), BF),
            pltpu.VMEM((half * side // 4, pairs, 16, lanes), BF),
            pltpu.VMEM((half * side * side * 3, 128), F32),
            pltpu.VMEM((4, 3 * 128, 128), F32),
            pltpu.SemaphoreType.DMA((len(pieces) + 5 + len(early) * planes,)),
        ],
        compiler_params=pltpu.CompilerParams(vmem_limit_bytes=VMEM_BYTES),
        cost_estimate=pl.CostEstimate(
            flops=20_000_000_000, bytes_accessed=25_000_000, transcendentals=0
        ),
        name="pair_coefficients",
    )(info, cells, signs, lines, *pieces, picks, *tables)


def coulomb_kernel(
    freq, shares, scale, own_first, info, keep, send, recv, w, *refs
):
    out, re, im, both, lhs, mixed, tiles, sems = refs[-8:]
    pairs, h_rows = re.shape
    g_rows = lhs.shape[1]
    tile = tiles.shape[2]
    steps = g_rows // tile
    wide, thin = pairs // 3, pairs // 6
    own = wide + thin
    cut = h_rows // CHUNKS

    def fetch(mine, columns, re_to, im_to, to_columns, base):
        copies = []
        for source, index in ((mine, info[1]), (recv, 1 - info[1])):
            for part, target in enumerate((re_to, im_to)):
                for row, to, n in (
                    (0, pl.multiple_of(index * wide, wide), wide),
                    (wide, pl.multiple_of(2 * wide + index * thin, thin), thin),
                ):
                    copies.append(
                        pltpu.make_async_copy(
                            source.at[pl.ds(part * own + row, n), columns],
                            target.at[pl.ds(to, n), to_columns],
                            sems.at[base + len(copies)],
                        )
                    )
        return copies

    def tile_copy(step, columns, slot, sem):
        rows = pl.ds(pl.multiple_of(step * tile, tile), tile)
        return pltpu.make_async_copy(
            w.at[freq, :, rows, columns], tiles.at[slot, :, :, columns], sems.at[sem]
        )

    whole = pl.ds(0, h_rows)
    spans = [pl.ds(k * cut, cut) for k in range(CHUNKS)]
    first = [
        fetch(keep, span, re, im, span, 10 * k) + [tile_copy(0, span, 0, 10 * k + 8)]
        for k, span in enumerate(spans)
    ]
    left = fetch(
        send,
        pl.ds(h_rows, g_rows),
        lhs.at[pl.ds(0, pairs)],
        lhs.at[pl.ds(pairs, pairs)],
        pl.ds(0, g_rows),
        10 * CHUNKS,
    )
    later = 10 * CHUNKS + 8

    for copies in first:
        for copy in copies:
            copy.start()
    tile_copy(1, whole, 1, later + 1).start()
    for copy in left:
        copy.start()

    def products(slot, columns):
        w_re, w_im = tiles[slot, 0, :, columns], tiles[slot, 1, :, columns]
        w_both = (w_re.astype(F32) + w_im.astype(F32)).astype(BF)
        return (
            dot_nt(re[:, columns], w_re),
            dot_nt(im[:, columns], w_im),
            dot_nt(both[:, columns], w_both),
        )

    def mix(step, re_re, im_im, all_all):
        at = pl.ds(pl.multiple_of(step * tile, tile), tile)
        mixed[:pairs, at] = (re_re - im_im).astype(BF)
        mixed[pairs:, at] = (all_all - re_re - im_im).astype(BF)

    total = None
    for span, copies in zip(spans, first):
        for copy in copies:
            copy.wait()
        both[:, span] = (re[:, span].astype(F32) + im[:, span].astype(F32)).astype(BF)
        terms = products(0, span)
        total = terms if total is None else tuple(a + b for a, b in zip(total, terms))
    mix(0, *total)

    def further(step, carry):
        slot = step & 1

        @pl.when(step + 1 < steps)
        def _():
            tile_copy(step + 1, whole, 1 - slot, later + 1 - slot).start()

        tile_copy(step, whole, slot, later + slot).wait()
        mix(step, *products(slot, whole))
        return carry

    lax.fori_loop(1, steps, further, 0)

    for copy in left:
        copy.wait()
    terms = dot_nt(lhs[...], mixed[...])
    u = (
        (terms[:pairs, :pairs] + terms[pairs:, pairs:]) * scale,
        (terms[:pairs, pairs:] - terms[pairs:, :pairs]) * scale,
    )
    n = pairs // shares
    for part in range(2):
        for s in range(shares):
            to = (s % 2 ^ info[1]) * (shares // 2) + s // 2 if own_first else s
            out[to, part] = u[part][s * n : (s + 1) * n].astype(BF)


def coulomb_partial(info, keep, send, recv, screened, freq, shares, scale, own_first, after):
    _, _, g_rows, h_rows = screened.shape
    pairs = keep.shape[0]
    tile = min(256, g_rows // 2)
    anywhere = pl.BlockSpec(memory_space=pl.ANY)
    return pl.pallas_call(
        functools.partial(coulomb_kernel, freq, shares, scale, own_first),
        out_shape=jax.ShapeDtypeStruct((shares, 2, pairs // shares, pairs), BF),
        in_specs=[pl.BlockSpec(memory_space=pltpu.SMEM)] + [anywhere] * (4 + len(after)),
        out_specs=pl.BlockSpec(memory_space=pltpu.VMEM),
        scratch_shapes=[
            pltpu.VMEM((pairs, h_rows), BF),
            pltpu.VMEM((pairs, h_rows), BF),
            pltpu.VMEM((pairs, h_rows), BF),
            pltpu.VMEM((2 * pairs, g_rows), BF),
            pltpu.VMEM((2 * pairs, g_rows), BF),
            pltpu.VMEM((2, 2, tile, h_rows), BF),
            pltpu.SemaphoreType.DMA((10 * CHUNKS + 10,)),
        ],
        compiler_params=pltpu.CompilerParams(vmem_limit_bytes=VMEM_BYTES),
        cost_estimate=pl.CostEstimate(
            flops=14_000_000_000, bytes_accessed=25_000_000, transcendentals=0
        ),
        name="coulomb_partial",
    )(info, keep, send, recv, screened, *after)


def cell_table(gmap, side):
    kx, ky, kz = gmap // (side * side), gmap // side % side, gmap % side
    mirrored = kz > side // 2
    kx, ky, kz = (jnp.where(mirrored, -k % side, k) for k in (kx, ky, kz))
    place = kx * 4 + ky % 4
    cells = (kz * (side // 4) + ky // 4) * 12 * side + place % (2 * side) * 6 + place // (2 * side)
    return cells, jnp.where(mirrored, -1.0, 1.0).astype(F32)


def shards(rows, cols, wannier, pairs, gmap, screened):
    members, _, grid_cells = wannier.shape
    side = math.isqrt(grid_cells)
    count = pairs.shape[0]
    waves = gmap.shape[0]
    g_rows, h_rows = screened.shape[2:]
    row, col = lax.axis_index("row"), lax.axis_index("col")
    info = jnp.stack([row, col]).astype(jnp.int32)
    swap = [(0, 1), (1, 0)]

    local = wannier.transpose(1, 0, 2)
    same = {0: local}
    for bit in reversed(range(log2(rows))):
        hop = [(i, i ^ (1 << bit)) for i in range(rows)]
        for shift in list(same):
            same[shift ^ (1 << bit)] = lax.ppermute(same[shift], "row", hop)
    cross = {}
    for shift in range(rows):
        cross[shift] = lax.ppermute(same[shift], "col", swap)

    wide = count // 3
    first = lax.dynamic_slice_in_dim(pairs, col * wide, wide, 0)
    last = lax.dynamic_slice_in_dim(pairs, 2 * wide + col * (wide // 2), wide // 2, 0)
    owned = jnp.concatenate([first, last], axis=0).T.reshape(-1, 1)
    picks = (owned == jnp.arange(2 * members, dtype=jnp.int32)[None, :] % members).astype(BF)

    norm = 1.0 / (math.sqrt(side**3) * SCALE**3)
    cells, signs = cell_table(gmap, side)

    def arranged(table):
        theirs = lax.dynamic_slice_in_dim(table, (1 - col) * h_rows, h_rows)
        block = lax.dynamic_slice_in_dim(table, row * g_rows, g_rows)
        ours = lax.dynamic_slice_in_dim(table, col * h_rows, h_rows)
        return jnp.concatenate([theirs, block, ours])

    cells, signs = arranged(cells), arranged(signs).reshape(-1, 128)
    info, cells, signs, picks = lax.optimization_barrier((info, cells, signs, picks))
    tables = stage_tables(side)
    early, late = tuple(range(rows // 2)), tuple(range(rows // 2, rows))

    def pieces(group):
        return [same[i] for i in group] + [cross[i] for i in group]

    lines = plane_lines(info, pieces(early), picks, tables[:3], side)
    send, keep = pair_coefficients(
        info, cells, signs, lines, pieces(late), picks, tables, early, late,
        side, norm, h_rows + g_rows,
    )
    recv = lax.ppermute(send, "col", swap)
    results, after = [], ()
    freqs = screened.shape[0]
    for freq in range(freqs):
        last = freq == freqs - 1
        partial = coulomb_partial(
            info, keep, send, recv, screened, freq, rows * cols, 1.0 / math.sqrt(waves), last, after
        )
        after = (partial,)
        axes = ("row", "col")
        if last:
            chip = partial[:rows].astype(F32) + lax.ppermute(partial[rows:], "col", swap)
            partial, axes = chip.astype(BF), "row"
        if results:
            partial, results[-1] = lax.optimization_barrier((partial, results[-1]))
        spread = lax.all_to_all(partial, axes, split_axis=0, concat_axis=0, tiled=True)
        results.append(jnp.sum(spread.astype(F32), axis=0))
    return jnp.stack(results)


def solution(mesh):
    rows, cols = mesh.shape["row"], mesh.shape["col"]

    def body(*arrays):
        return shards(rows, cols, *arrays)

    return jax.shard_map(
        body,
        mesh=mesh,
        in_specs=(P("kpt", ("row", "col"), None), P(), P(), P("kpt", None, "row", "col")),
        out_specs=P(None, None, ("kpt", "row", "col"), None),
        check_vma=False,
    )
```

```python
import functools
import math

import jax
import jax.numpy as jnp
import numpy as np
from jax import lax
from jax.experimental import pallas as pl
from jax.experimental.pallas import tpu as pltpu
from jax.sharding import PartitionSpec as P

BF = jnp.bfloat16
F32 = jnp.float32
SCALE = 1.62455
VMEM_BYTES = 67_043_328
CHUNKS = 4


def stage_tables(side):
    half = side // 2 + 1
    positions = np.arange(side)
    angles = 2.0 * np.pi * (np.outer(positions, positions) % side) / side
    cosine, sine = SCALE * np.cos(angles), SCALE * np.sin(angles)
    z_table = np.zeros((half, 2, 8, 8, side))
    for y in range(8):
        z_table[:, 0, y, y, :] = cosine[:half]
        z_table[:, 1, y, y, :] = -sine[:half]
    line = np.zeros((side, 2, side, 2))
    line[:, 0, :, 0] = cosine
    line[:, 0, :, 1] = sine
    line[:, 1, :, 0] = -sine
    line[:, 1, :, 1] = cosine
    y_one = line.reshape(side // 4, 4, 2, side // 8, 8, 2).transpose(0, 2, 1, 3, 5, 4)
    y_one = y_one.reshape(2 * side, 2 * side)
    x_four = np.einsum("koni,ab->okanib", line, np.eye(4)).reshape(8 * side, 8 * side)
    z_table = z_table.reshape(16 * half, 8 * side)
    tables = (z_table, np.kron(np.eye(4), y_one), y_one, x_four)
    return [jnp.asarray(table.astype(np.float32)).astype(BF) for table in tables]


def dot_nt(a, b):
    return lax.dot_general(a, b, (((1,), (1,)), ((), ())), preferred_element_type=F32)


def dot_nn(a, b):
    return lax.dot_general(a, b, (((1,), (0,)), ((), ())), preferred_element_type=F32)


def log2(n):
    return n.bit_length() - 1


def transform_planes(side, planes, my_col, pieces, tables, wann, mid1, sems, sink):
    picks, zt, yt, ys = [held for _, held in tables]
    half = side // 2 + 1
    lanes = mid1.shape[-1]
    own = lanes * 3 // 4
    shifts = len(pieces) // 2

    for index, piece in enumerate(pieces):
        at = pl.ds(index * planes, planes)
        pltpu.make_async_copy(piece, wann.at[at], sems.at[index]).start()
    loads = [
        pltpu.make_async_copy(table, held, sems.at[len(pieces) + index])
        for index, (table, held) in enumerate(tables)
    ]
    for load in loads:
        load.start()

    def arrived(index):
        at = pl.ds(index * planes, planes)
        pltpu.make_async_copy(pieces[0], wann.at[at], sems.at[index]).wait()

    def plane_pair(pair, carry):
        for h in range(2):
            x = 2 * pair + h
            shift = lax.shift_right_logical(x, log2(2 * planes))
            from_col = lax.shift_right_logical(x, log2(planes)) & 1
            index = (from_col ^ my_col) * shifts + shift
            if planes <= 2:
                if h % planes == 0:
                    arrived(index)
            else:
                pl.when(x & (planes - 1) == 0)(functools.partial(arrived, index))
            plane = wann[index * planes + (x & (planes - 1))]
            high = plane.astype(BF)
            low = (plane - high.astype(F32)).astype(BF)
            both = dot_nn(picks[...], jnp.concatenate([high, low], axis=0))
            density = (both[:own] * both[own:]).astype(BF)
            density = jnp.concatenate([density, density[lanes // 2 : own]], axis=0)
            for t in range(side // 8):
                lines = dot_nt(zt[...], density[:, t * 8 * side : (t + 1) * 8 * side])
                mid1[h, :, t] = lines.astype(BF).reshape(half, 16, lanes)
        target = sink(pair)
        for q in range(half // 4 + 1):
            parts = []
            for h in range(2):
                if q < half // 4:
                    lines = mid1[h, 4 * q : 4 * q + 4].reshape(8 * side, lanes)
                    parts.append(dot_nn(yt[...], lines))
                else:
                    parts.append(dot_nn(ys[...], mid1[h, half - 1].reshape(2 * side, lanes)))
            groups = parts[0].shape[0] // 8
            joined = jnp.concatenate([p.reshape(groups, 8, lanes) for p in parts], axis=1)
            target[pl.ds(q * side, groups)] = joined.astype(BF)
        return carry

    return plane_pair, loads


def plane_kernel(side, planes, info, *refs):
    pieces = refs[:-14]
    out, *held, wann, mid1, ready, sems, out_sems = refs[-10:]
    tables = list(zip(refs[-14:-10], held))
    pairs = len(pieces) // 2 * planes

    def put(pair):
        slot = pair & 1
        return pltpu.make_async_copy(ready.at[slot], out.at[pair], out_sems.at[slot])

    plane_pair, loads = transform_planes(
        side, planes, info[1], pieces, tables, wann, mid1, sems, lambda p: ready.at[p & 1]
    )
    for load in loads:
        load.wait()

    def step(pair, carry):
        pl.when(pair >= 2)(lambda: put(pair - 2).wait())
        plane_pair(pair, carry)
        put(pair).start()
        return carry

    lax.fori_loop(0, pairs, step, 0)
    for pair in range(max(pairs - 2, 0), pairs):
        put(pair).wait()


def plane_lines(info, pieces, picks, tables, side):
    planes, members = pieces[0].shape[:2]
    half = side // 2 + 1
    lanes = 256
    pairs = len(pieces) // 2 * planes
    return pl.pallas_call(
        functools.partial(plane_kernel, side, planes),
        out_shape=jax.ShapeDtypeStruct((pairs, half * side // 4, 16, lanes), BF),
        in_specs=[pl.BlockSpec(memory_space=pltpu.SMEM)]
        + [pl.BlockSpec(memory_space=pl.ANY)] * (len(pieces) + 4),
        out_specs=pl.BlockSpec(memory_space=pl.ANY),
        scratch_shapes=[pltpu.VMEM(table.shape, BF) for table in (picks, *tables)]
        + [
            pltpu.VMEM((2 * pairs, members, side * side), F32),
            pltpu.VMEM((2, half, side // 8, 16, lanes), BF),
            pltpu.VMEM((2, half * side // 4, 16, lanes), BF),
            pltpu.SemaphoreType.DMA((len(pieces) + 4,)),
            pltpu.SemaphoreType.DMA((2,)),
        ],
        compiler_params=pltpu.CompilerParams(vmem_limit_bytes=VMEM_BYTES),
        cost_estimate=pl.CostEstimate(
            flops=600_000_000 * pairs, bytes_accessed=6_000_000, transcendentals=0
        ),
        name="plane_lines",
    )(info, *pieces, picks, *tables)


def pair_kernel(side, planes, norm, early, late, info, cells, signs, *refs):
    early_lines, pieces = refs[0], refs[1:-21]
    send, keep, *held, xt, sent, kept, wann, mid1, mid2, spec, stages, sems, out_sems = refs[-16:]
    tables = list(zip(refs[-21:-16], held + [xt]))
    lanes = mid2.shape[-1]
    own = lanes * 3 // 4

    def place(shift, rest):
        return (info[0] ^ shift) * planes + rest

    copies = []
    for pair in range(len(early) * planes):
        to = place(early[pair // planes], pair % planes)
        copies.append(
            pltpu.make_async_copy(
                early_lines.at[pair], mid2.at[:, to], sems.at[len(pieces) + 5 + pair]
            )
        )
    plane_pair, loads = transform_planes(
        side, planes, info[1], pieces, tables[:4], wann, mid1, sems,
        lambda pair: mid2.at[:, place(late[0] + lax.div(pair, planes), pair & (planes - 1))],
    )
    copies.append(pltpu.make_async_copy(*tables[4], sems.at[len(pieces) + 4]))
    for copy in copies:
        copy.start()
    for load in loads:
        load.wait()
    lax.fori_loop(0, len(late) * planes, plane_pair, 0)
    for copy in copies:
        copy.wait()

    left = lax.broadcasted_iota(jnp.int32, (1, 128), 1) < 64

    def column(kq, carry):
        lines = dot_nn(xt[...], mid2[kq].reshape(8 * side, lanes))
        n = 4 * side
        re, im = lines[:n], lines[n:]
        thirds = (re[:, :128], im[:, :128], jnp.where(left, re[:, 128:], im[:, 128:]))
        for third in range(3):
            for odd in range(2):
                at = pl.ds(kq * 3 * n + 2 * third + odd, n // 2, stride=6)
                spec[at, :] = thirds[third][odd * n // 2 : (odd + 1) * n // 2]
        return carry

    lax.fori_loop(0, mid2.shape[0], column, 0, unroll=8)

    block = 128
    deep = stages.shape[0]

    def fill(slot, base):
        for j in range(block):
            odd, even = divmod(j, block // 2)
            row = spec[pl.ds(cells[base + j], 3, stride=2), :]
            stages[slot, pl.ds(6 * even + odd, 3, stride=2), :] = row

    def drain(slot, out, b, sign):
        at = pl.ds(pl.multiple_of(b * block, block), block)
        columns = []
        for third in range(3):
            halves = [
                stages[slot, pl.ds(2 * third + odd, block // 2, stride=6), :] for odd in range(2)
            ]
            whole = jnp.concatenate(halves, axis=0) * norm
            columns.append(jnp.transpose(whole.astype(BF)))
        half_rows = block // 2
        sign = sign.astype(BF)
        out[:block, at] = columns[0]
        out[block : block + half_rows, at] = columns[2][:half_rows]
        out[own : own + block, at] = columns[1] * sign
        out[own + block :, at] = columns[2][half_rows:] * sign

    def gather_into(held, out, first, base):
        width = deep * block

        def put(i):
            at = pl.ds(pl.multiple_of(i * width, width), width)
            return pltpu.make_async_copy(held.at[:, at], out.at[:, at], out_sems.at[base + i])

        def step(i, carry):
            for slot in range(deep):
                fill(slot, first + (i * deep + slot) * block)
            for slot in range(deep):
                b = i * deep + slot
                drain(slot, held, b, signs[pl.ds(first // block + b, 1), :])
            put(i).start()
            return carry

        steps = out.shape[1] // width
        lax.fori_loop(0, steps, step, 0)
        return [functools.partial(put, i) for i in range(steps)]

    puts = gather_into(sent, send, 0, 0)
    puts += gather_into(kept, keep, send.shape[1], len(puts))
    for put in puts:
        put().wait()


def pair_coefficients(
    info, cells, signs, lines, pieces, picks, tables, early, late, side, norm, send_rows
):
    keep_rows = cells.shape[0] - send_rows
    planes, members = pieces[0].shape[:2]
    half = side // 2 + 1
    lanes = 256
    pairs = side // 2
    smem = pl.BlockSpec(memory_space=pltpu.SMEM)
    vmem = pl.BlockSpec(memory_space=pltpu.VMEM)
    anywhere = pl.BlockSpec(memory_space=pl.ANY)
    return pl.pallas_call(
        functools.partial(pair_kernel, side, planes, norm, early, late),
        out_shape=(
            jax.ShapeDtypeStruct((384, send_rows), BF),
            jax.ShapeDtypeStruct((384, keep_rows), BF),
        ),
        in_specs=[smem, smem, vmem] + [anywhere] * (6 + len(pieces)),
        out_specs=(anywhere, anywhere),
        scratch_shapes=[pltpu.VMEM(table.shape, BF) for table in (picks, *tables)]
        + [
            pltpu.VMEM((384, send_rows), BF),
            pltpu.VMEM((384, keep_rows), BF),
            pltpu.VMEM((len(pieces) * planes, members, side * side), F32),
            pltpu.VMEM((2, half, side // 8, 16, lanes), BF),
            pltpu.VMEM((half * side // 4, pairs, 16, lanes), BF),
            pltpu.VMEM((half * side * side * 3, 128), F32),
            pltpu.VMEM((4, 3 * 128, 128), F32),
            pltpu.SemaphoreType.DMA((len(pieces) + 5 + len(early) * planes,)),
            pltpu.SemaphoreType.DMA(((send_rows + keep_rows) // 512,)),
        ],
        compiler_params=pltpu.CompilerParams(vmem_limit_bytes=VMEM_BYTES),
        cost_estimate=pl.CostEstimate(
            flops=20_000_000_000, bytes_accessed=25_000_000, transcendentals=0
        ),
        name="pair_coefficients",
    )(info, cells, signs, lines, *pieces, picks, *tables)


def coulomb_kernel(
    freq, shares, scale, own_first, info, keep, send, recv, w, *refs
):
    out, re, im, both, lhs, mixed, tiles, sems = refs[-8:]
    pairs, h_rows = re.shape
    g_rows = lhs.shape[1]
    tile = tiles.shape[2]
    steps = g_rows // tile
    wide, thin = pairs // 3, pairs // 6
    own = wide + thin
    cut = h_rows // CHUNKS

    def fetch(mine, columns, re_to, im_to, to_columns, base):
        copies = []
        for source, index in ((mine, info[1]), (recv, 1 - info[1])):
            for part, target in enumerate((re_to, im_to)):
                for row, to, n in (
                    (0, pl.multiple_of(index * wide, wide), wide),
                    (wide, pl.multiple_of(2 * wide + index * thin, thin), thin),
                ):
                    copies.append(
                        pltpu.make_async_copy(
                            source.at[pl.ds(part * own + row, n), columns],
                            target.at[pl.ds(to, n), to_columns],
                            sems.at[base + len(copies)],
                        )
                    )
        return copies

    def tile_copy(step, columns, slot, sem):
        rows = pl.ds(pl.multiple_of(step * tile, tile), tile)
        return pltpu.make_async_copy(
            w.at[freq, :, rows, columns], tiles.at[slot, :, :, columns], sems.at[sem]
        )

    whole = pl.ds(0, h_rows)
    spans = [pl.ds(k * cut, cut) for k in range(CHUNKS)]
    first = [
        fetch(keep, span, re, im, span, 10 * k) + [tile_copy(0, span, 0, 10 * k + 8)]
        for k, span in enumerate(spans)
    ]
    left = fetch(
        send,
        pl.ds(h_rows, g_rows),
        lhs.at[pl.ds(0, pairs)],
        lhs.at[pl.ds(pairs, pairs)],
        pl.ds(0, g_rows),
        10 * CHUNKS,
    )
    later = 10 * CHUNKS + 8

    for copies in first:
        for copy in copies:
            copy.start()
    tile_copy(1, whole, 1, later + 1).start()
    for copy in left:
        copy.start()

    def products(slot, columns):
        w_re, w_im = tiles[slot, 0, :, columns], tiles[slot, 1, :, columns]
        w_both = (w_re.astype(F32) + w_im.astype(F32)).astype(BF)
        return (
            dot_nt(re[:, columns], w_re),
            dot_nt(im[:, columns], w_im),
            dot_nt(both[:, columns], w_both),
        )

    def mix(step, re_re, im_im, all_all):
        at = pl.ds(pl.multiple_of(step * tile, tile), tile)
        mixed[:pairs, at] = (re_re - im_im).astype(BF)
        mixed[pairs:, at] = (all_all - re_re - im_im).astype(BF)

    total = None
    for span, copies in zip(spans, first):
        for copy in copies:
            copy.wait()
        both[:, span] = (re[:, span].astype(F32) + im[:, span].astype(F32)).astype(BF)
        terms = products(0, span)
        total = terms if total is None else tuple(a + b for a, b in zip(total, terms))
    mix(0, *total)

    def further(step, carry):
        slot = step & 1

        @pl.when(step + 1 < steps)
        def _():
            tile_copy(step + 1, whole, 1 - slot, later + 1 - slot).start()

        tile_copy(step, whole, slot, later + slot).wait()
        mix(step, *products(slot, whole))
        return carry

    lax.fori_loop(1, steps, further, 0)

    for copy in left:
        copy.wait()
    terms = dot_nt(lhs[...], mixed[...])
    u = (
        (terms[:pairs, :pairs] + terms[pairs:, pairs:]) * scale,
        (terms[:pairs, pairs:] - terms[pairs:, :pairs]) * scale,
    )
    n = pairs // shares
    for part in range(2):
        for s in range(shares):
            to = (s % 2 ^ info[1]) * (shares // 2) + s // 2 if own_first else s
            out[to, part] = u[part][s * n : (s + 1) * n].astype(BF)


def coulomb_partial(info, keep, send, recv, screened, freq, shares, scale, own_first, after):
    _, _, g_rows, h_rows = screened.shape
    pairs = keep.shape[0]
    tile = min(256, g_rows // 2)
    anywhere = pl.BlockSpec(memory_space=pl.ANY)
    return pl.pallas_call(
        functools.partial(coulomb_kernel, freq, shares, scale, own_first),
        out_shape=jax.ShapeDtypeStruct((shares, 2, pairs // shares, pairs), BF),
        in_specs=[pl.BlockSpec(memory_space=pltpu.SMEM)] + [anywhere] * (4 + len(after)),
        out_specs=pl.BlockSpec(memory_space=pltpu.VMEM),
        scratch_shapes=[
            pltpu.VMEM((pairs, h_rows), BF),
            pltpu.VMEM((pairs, h_rows), BF),
            pltpu.VMEM((pairs, h_rows), BF),
            pltpu.VMEM((2 * pairs, g_rows), BF),
            pltpu.VMEM((2 * pairs, g_rows), BF),
            pltpu.VMEM((2, 2, tile, h_rows), BF),
            pltpu.SemaphoreType.DMA((10 * CHUNKS + 10,)),
        ],
        compiler_params=pltpu.CompilerParams(vmem_limit_bytes=VMEM_BYTES),
        cost_estimate=pl.CostEstimate(
            flops=14_000_000_000, bytes_accessed=25_000_000, transcendentals=0
        ),
        name="coulomb_partial",
    )(info, keep, send, recv, screened, *after)


def cell_table(gmap, side):
    kx, ky, kz = gmap // (side * side), gmap // side % side, gmap % side
    mirrored = kz > side // 2
    kx, ky, kz = (jnp.where(mirrored, -k % side, k) for k in (kx, ky, kz))
    place = kx * 4 + ky % 4
    cells = (kz * (side // 4) + ky // 4) * 12 * side + place % (2 * side) * 6 + place // (2 * side)
    return cells, jnp.where(mirrored, -1.0, 1.0).astype(F32)


def shards(rows, cols, wannier, pairs, gmap, screened):
    members, _, grid_cells = wannier.shape
    side = math.isqrt(grid_cells)
    count = pairs.shape[0]
    waves = gmap.shape[0]
    g_rows, h_rows = screened.shape[2:]
    row, col = lax.axis_index("row"), lax.axis_index("col")
    info = jnp.stack([row, col]).astype(jnp.int32)
    swap = [(0, 1), (1, 0)]

    local = wannier.transpose(1, 0, 2)
    same = {0: local}
    for bit in reversed(range(log2(rows))):
        hop = [(i, i ^ (1 << bit)) for i in range(rows)]
        for shift in list(same):
            same[shift ^ (1 << bit)] = lax.ppermute(same[shift], "row", hop)
    cross = {}
    for shift in range(rows):
        cross[shift] = lax.ppermute(same[shift], "col", swap)

    wide = count // 3
    first = lax.dynamic_slice_in_dim(pairs, col * wide, wide, 0)
    last = lax.dynamic_slice_in_dim(pairs, 2 * wide + col * (wide // 2), wide // 2, 0)
    owned = jnp.concatenate([first, last], axis=0).T.reshape(-1, 1)
    picks = (owned == jnp.arange(2 * members, dtype=jnp.int32)[None, :] % members).astype(BF)

    norm = 1.0 / (math.sqrt(side**3) * SCALE**3)
    cells, signs = cell_table(gmap, side)

    def arranged(table):
        theirs = lax.dynamic_slice_in_dim(table, (1 - col) * h_rows, h_rows)
        block = lax.dynamic_slice_in_dim(table, row * g_rows, g_rows)
        ours = lax.dynamic_slice_in_dim(table, col * h_rows, h_rows)
        return jnp.concatenate([theirs, block, ours])

    cells, signs = arranged(cells), arranged(signs).reshape(-1, 128)
    info, cells, signs, picks = lax.optimization_barrier((info, cells, signs, picks))
    tables = stage_tables(side)
    early, late = tuple(range(rows // 2)), tuple(range(rows // 2, rows))

    def pieces(group):
        return [same[i] for i in group] + [cross[i] for i in group]

    lines = plane_lines(info, pieces(early), picks, tables[:3], side)
    send, keep = pair_coefficients(
        info, cells, signs, lines, pieces(late), picks, tables, early, late,
        side, norm, h_rows + g_rows,
    )
    recv = lax.ppermute(send, "col", swap)
    results, after = [], ()
    freqs = screened.shape[0]
    for freq in range(freqs):
        last = freq == freqs - 1
        partial = coulomb_partial(
            info, keep, send, recv, screened, freq, rows * cols, 1.0 / math.sqrt(waves), last, after
        )
        after = (partial,)
        axes = ("row", "col")
        if last:
            chip = partial[:rows].astype(F32) + lax.ppermute(partial, "col", swap)[rows:]
            partial, axes = chip.astype(BF), "row"
        if results:
            partial, results[-1] = lax.optimization_barrier((partial, results[-1]))
        spread = lax.all_to_all(partial, axes, split_axis=0, concat_axis=0, tiled=True)
        results.append(jnp.sum(spread.astype(F32), axis=0))
    return jnp.stack(results)


def solution(mesh):
    rows, cols = mesh.shape["row"], mesh.shape["col"]

    def body(*arrays):
        return shards(rows, cols, *arrays)

    return jax.shard_map(
        body,
        mesh=mesh,
        in_specs=(P("kpt", ("row", "col"), None), P(), P(), P("kpt", None, "row", "col")),
        out_specs=P(None, None, ("kpt", "row", "col"), None),
        check_vma=False,
    )
```
